32 devices in a mesh: dp: 8 (over z, core), section: 4 (over y, x).
Axes of the slice: x: 2, y: 2, z: 4, core: 2. Of those that a mesh axis runs over, the one named last changes fastest.
Arguments:
- hidden_act: bfloat16 [1024, 14336], P('dp', 'section'), may hold values from -6 to 6
- out_grad: bfloat16 [1024, 4608], P('dp'), may hold values from -0.1875 to 0.1875
- grad_accum: float32 [14336, 4608], P('section', 'dp'), may hold values from -6 to 6
- master_weight: float32 [14336, 4608], P('section', 'dp'), may hold values from -0.046875 to 0.046875
- adam_first: float32 [14336, 4608], P('section', 'dp'), may hold values from -2 to 2
- adam_second: float32 [14336, 4608], P('section', 'dp'), may hold values from 0.1 to 10
- decode_in: bfloat16 [4, 128, 14336], P(None, 'dp', 'section'), may hold values from -6 to 6
- residual_in: bfloat16 [4, 128, 4608], P(None, 'dp'), may hold values from -6 to 6
- norm_gain: bfloat16 [4608], P('section'), may hold values from 0.25 to 1.75
Outputs:
- weight_new: float32 [14336, 4608], P('section', 'dp')
- first_new: float32 [14336, 4608], P('section', 'dp')
- second_new: float32 [14336, 4608], P('section', 'dp')
- decoded: bfloat16 [4, 128, 4608], P(None, 'dp', 'section')
The draws below stay inside these ranges and needn't reach their ends.
All inputs are finite; a program needn't handle non-finite values.
Results may differ from the reference program's by a relative error of at most 0.0039.
Values may be sent and summed in bfloat16 or wider, within the bound.
No kernel may reach another device: no remote copies, remote signals or barrier semaphores. Data moves between devices by JAX's collectives and lax.ppermute only.
A program may use at most 192 MiB of HBM per device.

```python
import math
import jax
import jax.numpy as jnp
from jax import lax

D = 4608
FF = 14336
STEPS = 4
TOKENS = 1024
ROLLOUT = 128


def spiked(values, rng, source, target, blocks, factor):
    owner, partner = [(jnp.arange(values.shape[position]) // (values.shape[position] // blocks)).reshape([-1 if axis == position else 1 for axis in range(values.ndim)]) for position in (source, target)]
    chosen = jax.random.permutation(rng, blocks)[partner]
    strong = (owner == chosen) | (owner == (partner + blocks // 2) % blocks)
    return jnp.where(strong, factor * values, values)


def shard_levels(own_key, dims, cuts, low, top_value):
    def one(axis_at, shards_of):
        steps = jax.random.uniform(jax.random.fold_in(jax.random.fold_in(own_key, 6), axis_at), (shards_of,), jnp.float32, low / len(cuts), top_value / len(cuts))
        return jnp.repeat(jnp.exp(steps), dims[axis_at] // shards_of).reshape((-1,) + (1,) * (len(dims) - axis_at - 1))

    loudness = one(*cuts[0])
    for cut in cuts[1:]:
        loudness = loudness * one(*cut)
    return loudness


def noise(own_key, shape, spread, limit, split=(), held_as=jnp.bfloat16):
    drawn = jax.random.normal(own_key, shape, jnp.float32) * spread
    if len(split) > 0:
        drawn = shard_levels(own_key, shape, split, -0.22, 0.18) * drawn
    return jnp.clip(drawn, min=-limit, max=limit).astype(held_as)


def noise_with(key, dims, deviation, most, pieces, heavy, kind=jnp.bfloat16):
    entries = deviation * jax.random.normal(key, dims, jnp.float32)
    if pieces:
        entries = entries * shard_levels(key, dims, pieces, -0.22, 0.18)
    return jnp.clip(spiked(entries, jax.random.fold_in(key, 3), *heavy), -most, most).astype(kind)


def setup_inputs(seed: int = 0) -> dict:
    streams_of = jax.random.split(jax.random.key(seed), 10)
    return {
        "hidden_act": noise(streams_of[0], (TOKENS, FF), 1.0, 6.0, ((0, 8), (1, 4))),
        "out_grad": noise_with(streams_of[1], (TOKENS, D), (TOKENS ** -0.5), 0.1875, ((0, 8),), (0, 1, 8, 2.0)),
        "grad_accum": noise(streams_of[2], (FF, D), 1.0, 6.0, ((0, 4), (1, 8)), jnp.float32),
        "master_weight": noise(streams_of[3], (FF, D), FF ** -0.5, 0.046875, ((0, 4), (1, 8)), jnp.float32),
        "adam_first": noise(streams_of[4], (FF, D), 0.3, 2.0, ((0, 4), (1, 8)), jnp.float32),
        "adam_second": jnp.clip(jnp.exp(math.log(10.0) - 4.6051702 * jax.random.uniform(streams_of[5], (FF, D), jnp.float32) ** shard_levels(streams_of[5], (FF, D), ((0, 4), (1, 8)), -0.2, 0.2)), 0.1, 10.0),
        "decode_in": noise(streams_of[6], (STEPS, ROLLOUT, FF), 1.0, 6.0, ((1, 8), (2, 4))),
        "residual_in": noise(streams_of[7], (STEPS, ROLLOUT, D), 1.0, 6.0, ((1, 8),)),
        "norm_gain": jnp.clip(1.0 + 0.15 * jax.random.normal(streams_of[8], (D,), jnp.float32), 0.25, 1.75).astype(jnp.bfloat16),
    }


beta_first = 0.9
beta_second = 0.95
learn_rate = 0.002
decay_rate = 0.1
adam_eps = 1e-08
norm_eps = 1e-05
bias_first = 1.0 - 0.9 ** 10
bias_second = 1.0 - 0.95 ** 10

def reference(hidden_act, out_grad, grad_accum, master_weight, adam_first, adam_second, decode_in, residual_in, norm_gain):
    gradient = jnp.dot(hidden_act.T, out_grad, preferred_element_type=jnp.float32) + grad_accum
    first_new = beta_first * adam_first + (1.0 - beta_first) * gradient
    second_new = beta_second * adam_second + (1.0 - beta_second) * gradient * gradient
    update = first_new / bias_first / (jnp.sqrt(second_new / bias_second) + adam_eps)
    weight_new = master_weight - learn_rate * (update + decay_rate * master_weight)
    weight_rounded = weight_new.astype(jnp.bfloat16)
    flat_in = decode_in.reshape(STEPS * ROLLOUT, FF)
    stream = residual_in.reshape(STEPS * ROLLOUT, D).astype(jnp.float32) + jnp.dot(flat_in, weight_rounded, preferred_element_type=jnp.float32)
    mean_square = lax.optimization_barrier(jnp.mean(stream * stream, axis=1, keepdims=True))
    normed = stream * lax.rsqrt(mean_square + norm_eps) * norm_gain.astype(jnp.float32)
    decoded = normed.astype(jnp.bfloat16).reshape(STEPS, ROLLOUT, D)
    return (weight_new, first_new, second_new, decoded)
```

```python
import functools

import jax
import jax.numpy as jnp
from jax import lax
from jax.experimental import pallas as pl
from jax.experimental.pallas import tpu as pltpu
from jax.sharding import PartitionSpec as P

beta_first = 0.9
beta_second = 0.95
learn_rate = 0.002
decay_rate = 0.1
adam_eps = 1e-08
norm_eps = 1e-05
bias_first = 1.0 - 0.9**10
bias_second = 1.0 - 0.95**10


def ring_place(index, length):
    return jnp.where(2 * index < length, 2 * index, 2 * (length - index) - 1)


def ring_index(place, length):
    return jnp.where(place % 2 == 0, place // 2, length - (place + 1) // 2)


def ring_order(length):
    return [2 * i if 2 * i < length else 2 * (length - i) - 1 for i in range(length)]


def ring_pairs(length, cores, step):
    order = ring_order(length)
    return [
        (order[i] * cores + c, order[(i + step) % length] * cores + c)
        for i in range(length)
        for c in range(cores)
    ]


def ring_gather(own, length, cores):
    found = [(0, own)]
    up, down = own, own
    for step in range(1, (length - 1) // 2 + 1):
        up = lax.ppermute(up, "dp", ring_pairs(length, cores, 1))
        down = lax.ppermute(down, "dp", ring_pairs(length, cores, -1))
        found += [(-step, up), (step, down)]
    if length % 2 == 0:
        half = own.shape[0] // 2
        first = lax.ppermute(up[:half], "dp", ring_pairs(length, cores, 1))
        second = lax.ppermute(down[half:], "dp", ring_pairs(length, cores, -1))
        found += [(length // 2, (first, second))]
    return found


def chip_gather(own, length, cores):
    found = [(0, offset, block) for offset, block in ring_gather(own, length, cores)]
    if cores == 2:
        swap = [(i, i ^ 1) for i in range(length * cores)]
        found += [
            (1, offset, jax.tree.map(lambda part: lax.ppermute(part, "dp", swap), block))
            for _, offset, block in found
        ]
    return found


def pick_tile(size, most):
    fits = [t for t in range(128, most + 1, 128) if size % t == 0]
    return fits[-1] if fits else size


def update_body(count, grad_ref, *refs):
    acts, (accum, weight, first, second), (w_out, f_out, s_out, r_out) = (
        refs[:count],
        refs[count : count + 4],
        refs[count + 4 :],
    )
    act = jnp.concatenate([ref[...] for ref in acts], axis=0)
    gradient = jnp.dot(grad_ref[...], act, preferred_element_type=jnp.float32) + accum[...]
    first_new = beta_first * first[...] + (1.0 - beta_first) * gradient
    second_new = beta_second * second[...] + (1.0 - beta_second) * gradient * gradient
    scale = jnp.sqrt(second_new * (1.0 / bias_second)) + adam_eps
    update = first_new * (1.0 / bias_first) / scale
    old = weight[...]
    weight_new = old - learn_rate * (update + decay_rate * old)
    w_out[...] = weight_new
    f_out[...] = first_new
    s_out[...] = second_new
    r_out[...] = weight_new.astype(jnp.bfloat16)


def update_weights(grad_t, acts, accum_t, weight_t, first_t, second_t):
    width, hidden = accum_t.shape
    tile = pick_tile(hidden, 512)
    state = pl.BlockSpec((width, tile), lambda i: (0, i))
    return pl.pallas_call(
        functools.partial(update_body, len(acts)),
        grid=(hidden // tile,),
        in_specs=[pl.BlockSpec(grad_t.shape, lambda i: (0, 0))]
        + [pl.BlockSpec((act.shape[0], tile), lambda i: (0, i)) for act in acts]
        + [state] * 4,
        out_specs=[state] * 4,
        out_shape=[jax.ShapeDtypeStruct((width, hidden), jnp.float32)] * 3
        + [jax.ShapeDtypeStruct((width, hidden), jnp.bfloat16)],
        cost_estimate=pl.CostEstimate(
            flops=2 * grad_t.shape[1] * width * hidden,
            bytes_accessed=30 * width * hidden,
            transcendentals=2 * width * hidden,
        ),
        name="update_weights",
    )(grad_t, *acts, accum_t, weight_t, first_t, second_t)


def decode_body(plan, rows, places, *refs):
    count = sum(len(parts) for parts in plan)
    acts, weight, out, total = refs[:count], refs[count], refs[count + 1], refs[count + 2]
    step = pl.program_id(0)
    act = jnp.concatenate([ref[...] for ref in acts], axis=0)
    term = lax.dot_general(
        act, weight[...], (((1,), (1,)), ((), ())), preferred_element_type=jnp.float32
    )

    @pl.when(step == 0)
    def _():
        total[...] = term

    @pl.when(step > 0)
    def _():
        total[...] += term

    @pl.when(step == pl.num_programs(0) - 1)
    def _():
        for block in range(len(plan)):
            out[places[block]] = total[block * rows : (block + 1) * rows, :]


def decode_partial(places, plan, acts, weight_t):
    width, hidden = weight_t.shape
    tile = pick_tile(hidden, 512)
    blocks = len(plan)
    rows = sum(act.shape[0] for act in acts) // blocks
    return pl.pallas_call(
        functools.partial(decode_body, plan, rows),
        grid_spec=pltpu.PrefetchScalarGridSpec(
            num_scalar_prefetch=1,
            grid=(hidden // tile,),
            in_specs=[pl.BlockSpec((act.shape[0], tile), lambda i, p: (0, i)) for act in acts]
            + [pl.BlockSpec((width, tile), lambda i, p: (0, i))],
            out_specs=pl.BlockSpec((blocks, rows, width), lambda i, p: (0, 0, 0)),
            scratch_shapes=[pltpu.VMEM((blocks * rows, width), jnp.float32)],
        ),
        out_shape=jax.ShapeDtypeStruct((blocks, rows, width), jnp.float32),
        cost_estimate=pl.CostEstimate(
            flops=2 * blocks * rows * width * hidden,
            bytes_accessed=2 * hidden * (width + blocks * rows),
            transcendentals=0,
        ),
        name="decode_partial",
    )(places, *acts, weight_t)


def flat_parts(found):
    plan, parts = [], []
    for _, _, block in found:
        leaves = jax.tree.leaves(block)
        plan.append(leaves)
        parts += leaves
    return [tuple(leaf.shape[0] for leaf in leaves) for leaves in plan], parts


def section_sum(value):
    count = lax.axis_size("section")
    if count & (count - 1):
        return lax.psum(value, "section")
    step = 1
    while step < count:
        value = value + lax.ppermute(value, "section", [(i, i ^ step) for i in range(count)])
        step *= 2
    return value


def per_device(
    hidden_act,
    out_grad,
    grad_accum,
    master_weight,
    adam_first,
    adam_second,
    decode_in,
    residual_in,
    norm_gain,
):
    n_dp, n_sec = lax.axis_size("dp"), lax.axis_size("section")
    me, col = lax.axis_index("dp"), lax.axis_index("section")
    cores = 2 if n_dp % 2 == 0 else 1
    length = n_dp // cores
    chip, core = me // cores, me % cores
    spot = ring_index(chip, length)
    tokens, width_all = out_grad.shape
    steps_count, roll_rows, hidden_local = decode_in.shape
    rows = steps_count * roll_rows
    width = width_all // n_dp
    share_width = width_all // n_sec

    acts = chip_gather(hidden_act, length, cores)
    flat_in = decode_in.reshape(rows, hidden_local)
    decs = chip_gather(flat_in, length, cores)
    sources = jnp.stack(
        [
            ring_place((spot + offset) % length, length) * cores + (core ^ other)
            for other, offset, _ in acts
        ]
    ).astype(jnp.int32)

    part = tokens // n_sec
    mine = lax.dynamic_slice_in_dim(out_grad, col * part, part, 0)
    mine = mine.reshape(part, n_dp, width).transpose(1, 0, 2)
    got = lax.all_to_all(mine, "dp", 0, 0, tiled=True)
    pieces = [got] + [
        lax.ppermute(got, "section", [(i, (i + k) % n_sec) for i in range(n_sec)])
        for k in range(1, n_sec)
    ]
    order = (col - jnp.arange(n_sec)) % n_sec
    grads = jnp.stack(pieces)[order]
    grads = grads.transpose(1, 0, 2, 3).reshape(n_dp, tokens, width)[sources]
    grad_t = grads.reshape(n_dp * tokens, width).T

    _, act_parts = flat_parts(acts)
    weight_t, first_t, second_t, rounded_t = update_weights(
        grad_t, act_parts, grad_accum.T, master_weight.T, adam_first.T, adam_second.T
    )

    plan, dec_parts = flat_parts(decs)
    resid = lax.dynamic_slice_in_dim(
        residual_in.reshape(rows, width_all), col * share_width, share_width, 1
    ).astype(jnp.float32)
    if length == n_sec:
        places = ((sources // cores - col) % n_sec) * cores + ((sources % cores) ^ core)
        partial_out = decode_partial(places, plan, dec_parts, rounded_t)
        partial_out = partial_out.reshape(n_sec, cores, rows, width)
        summed = partial_out[0]
        for k in range(1, n_sec):
            summed = summed + lax.ppermute(
                partial_out[k], "section", [(i, (i + k) % n_sec) for i in range(n_sec)]
            )
        moved = []
        for j in range(cores):
            pairs = [
                ((a * cores + b) * n_sec + s, (s * cores + (b ^ j)) * n_sec + a)
                for a in range(length)
                for b in range(cores)
                for s in range(n_sec)
            ]
            moved.append(lax.ppermute(summed[j], ("dp", "section"), pairs))
        if cores == 2:
            flip = core == 1
            moved = [jnp.where(flip, moved[1], moved[0]), jnp.where(flip, moved[0], moved[1])]
        own_stream = resid + jnp.concatenate(moved, axis=1)
    else:
        partial_out = decode_partial(sources, plan, dec_parts, rounded_t)
        back = lax.all_to_all(partial_out, "dp", 0, 0, tiled=True)
        back = back.transpose(1, 0, 2).reshape(rows, width_all)
        own_stream = resid + lax.psum_scatter(back, "section", scatter_dimension=1, tiled=True)

    square_sum = section_sum(jnp.sum(own_stream * own_stream, axis=1, keepdims=True))
    mean_square = square_sum / width_all
    normed = own_stream * lax.rsqrt(mean_square + norm_eps) * norm_gain.astype(jnp.float32)
    decoded = normed.astype(jnp.bfloat16).reshape(steps_count, roll_rows, share_width)
    return (weight_t.T, first_t.T, second_t.T, decoded)


def solution(mesh):
    return jax.shard_map(
        per_device,
        mesh=mesh,
        in_specs=(
            P("dp", "section"),
            P("dp", None),
            P("section", "dp"),
            P("section", "dp"),
            P("section", "dp"),
            P("section", "dp"),
            P(None, "dp", "section"),
            P(None, "dp", None),
            P("section"),
        ),
        out_specs=(
            P("section", "dp"),
            P("section", "dp"),
            P("section", "dp"),
            P(None, "dp", "section"),
        ),
        check_vma=False,
    )
```

```python
import functools

import jax
import jax.numpy as jnp
from jax import lax
from jax.experimental import pallas as pl
from jax.experimental.pallas import tpu as pltpu
from jax.sharding import PartitionSpec as P


beta_first = 0.9
beta_second = 0.95
learn_rate = 0.002
decay_rate = 0.1
adam_eps = 1e-08
norm_eps = 1e-05
bias_first = 1.0 - 0.9**10
bias_second = 1.0 - 0.95**10


def ring_place(index, length):
    return jnp.where(2 * index < length, 2 * index, 2 * (length - index) - 1)


def ring_index(place, length):
    return jnp.where(place % 2 == 0, place // 2, length - (place + 1) // 2)


def ring_order(length):
    return [2 * i if 2 * i < length else 2 * (length - i) - 1 for i in range(length)]


def ring_pairs(length, cores, step):
    order = ring_order(length)
    return [
        (order[i] * cores + c, order[(i + step) % length] * cores + c)
        for i in range(length)
        for c in range(cores)
    ]


def ring_gather(own, length, cores):
    found = [(0, own)]
    up, down = own, own
    for step in range(1, (length - 1) // 2 + 1):
        up = lax.ppermute(up, "dp", ring_pairs(length, cores, 1))
        down = lax.ppermute(down, "dp", ring_pairs(length, cores, -1))
        found += [(-step, up), (step, down)]
    if length % 2 == 0:
        up = lax.ppermute(up, "dp", ring_pairs(length, cores, 1))
        found += [(length // 2, up)]
    return found


def chip_gather(own, length, cores):
    found = [(0, offset, block) for offset, block in ring_gather(own, length, cores)]
    if cores == 2:
        swap = [(i, i ^ 1) for i in range(length * cores)]
        for _, offset, block in list(found):
            found.append((1, offset, lax.ppermute(block, "dp", swap)))
    return found


def pick_tile(size, most):
    fits = [t for t in range(128, most + 1, 128) if size % t == 0]
    return fits[-1] if fits else size


def pick_spans(hidden, split):
    tile = pick_tile(hidden, 512)
    count = hidden // tile
    small = 2 * count // 7
    if not split or small == 0:
        return tile, [hidden]
    return tile, [(count - 2 * small) * tile, small * tile, small * tile]


def update_body(count, grad_ref, *refs):
    acts, (accum, weight, first, second) = refs[:count], refs[count : count + 4]
    w_out, f_out, s_out, r_out = refs[-4:]
    act = jnp.concatenate([ref[...] for ref in acts], axis=0)
    gradient = jnp.dot(grad_ref[...], act, preferred_element_type=jnp.float32) + accum[...]
    first_new = beta_first * first[...] + (1.0 - beta_first) * gradient
    second_new = beta_second * second[...] + (1.0 - beta_second) * gradient * gradient
    scale = jnp.sqrt(second_new * (1.0 / bias_second)) + adam_eps
    update = first_new * (1.0 / bias_first) / scale
    old = weight[...]
    weight_new = old - learn_rate * (update + decay_rate * old)
    w_out[...] = weight_new
    f_out[...] = first_new
    s_out[...] = second_new
    r_out[...] = weight_new.astype(jnp.bfloat16)


def update_weights(grad_t, acts, state, done, start, tile):
    width, hidden = state[0].shape
    span = acts[0].shape[1]
    skip = start // tile
    block = pl.BlockSpec((width, tile), lambda i: (0, i + skip))
    return pl.pallas_call(
        functools.partial(update_body, len(acts)),
        grid=(span // tile,),
        in_specs=[pl.BlockSpec(grad_t.shape, lambda i: (0, 0))]
        + [pl.BlockSpec((act.shape[0], tile), lambda i: (0, i)) for act in acts]
        + [block] * 4
        + [pl.BlockSpec(memory_space=pl.ANY)] * len(done),
        out_specs=[block] * 4,
        out_shape=[jax.ShapeDtypeStruct((width, hidden), jnp.float32)] * 3
        + [jax.ShapeDtypeStruct((width, hidden), jnp.bfloat16)],
        input_output_aliases={5 + len(acts) + i: i for i in range(len(done))},
        cost_estimate=pl.CostEstimate(
            flops=2 * grad_t.shape[1] * width * span,
            bytes_accessed=30 * width * span,
            transcendentals=2 * width * span,
        ),
        name="update_weights",
    )(grad_t, *acts, *state, *done)


def decode_body(count, rows, places, *refs):
    acts, weight, outs = refs[:count], refs[count], refs[count + 1 : -2]
    total, placed = refs[-2:]
    step = pl.program_id(0)
    act = jnp.concatenate([ref[...] for ref in acts], axis=0)
    term = lax.dot_general(
        act, weight[...], (((1,), (1,)), ((), ())), preferred_element_type=jnp.float32
    )

    @pl.when(step == 0)
    def _():
        total[...] = term

    @pl.when(step > 0)
    def _():
        total[...] += term

    @pl.when(step == pl.num_programs(0) - 1)
    def _():
        for block in range(count):
            placed[places[block]] = total[block * rows : (block + 1) * rows, :]
        each = count // len(outs)
        for i, out in enumerate(outs):
            out[...] = placed[i * each : (i + 1) * each]


def decode_partial(places, acts, weight_t, groups):
    width, hidden = weight_t.shape
    tile = pick_tile(hidden, hidden // 2)
    blocks, rows = len(acts), acts[0].shape[0]
    return pl.pallas_call(
        functools.partial(decode_body, blocks, rows),
        grid_spec=pltpu.PrefetchScalarGridSpec(
            num_scalar_prefetch=1,
            grid=(hidden // tile,),
            in_specs=[pl.BlockSpec((act.shape[0], tile), lambda i, p: (0, i)) for act in acts]
            + [pl.BlockSpec((width, tile), lambda i, p: (0, i))],
            out_specs=[pl.BlockSpec((blocks // groups, rows, width), lambda i, p: (0, 0, 0))] * groups,
            scratch_shapes=[
                pltpu.VMEM((blocks * rows, width), jnp.float32),
                pltpu.VMEM((blocks, rows, width), jnp.float32),
            ],
        ),
        out_shape=[jax.ShapeDtypeStruct((blocks // groups, rows, width), jnp.float32)] * groups,
        cost_estimate=pl.CostEstimate(
            flops=2 * blocks * rows * width * hidden,
            bytes_accessed=2 * hidden * (width + blocks * rows),
            transcendentals=0,
        ),
        name="decode_partial",
    )(places, *acts, weight_t)


def section_sum(value):
    count = lax.axis_size("section")
    if count & (count - 1):
        return lax.psum(value, "section")
    step = 1
    while step < count:
        value = value + lax.ppermute(value, "section", [(i, i ^ step) for i in range(count)])
        step *= 2
    return value


def per_device(
    hidden_act,
    out_grad,
    grad_accum,
    master_weight,
    adam_first,
    adam_second,
    decode_in,
    residual_in,
    norm_gain,
):
    n_dp, n_sec = lax.axis_size("dp"), lax.axis_size("section")
    me, col = lax.axis_index("dp"), lax.axis_index("section")
    cores = 2 if n_dp % 2 == 0 else 1
    length = n_dp // cores
    chip, core = me // cores, me % cores
    spot = ring_index(chip, length)
    tokens, width_all = out_grad.shape
    steps_count, roll_rows, hidden_local = decode_in.shape
    rows = steps_count * roll_rows
    width = width_all // n_dp
    share_width = width_all // n_sec

    tile, spans = pick_spans(hidden_local, length == n_sec)
    pieces = len(spans)
    starts = [sum(spans[:i]) for i in range(pieces)]
    chunks = 2 if length == n_sec else 1
    cut = rows // chunks
    acts, decs = [], []
    for i in range(pieces):
        own = hidden_act[:, starts[i] : starts[i] + spans[i]]
        acts.append(chip_gather(own, length, cores))
    flat_in = decode_in.reshape(rows, hidden_local)
    for i in range(chunks):
        decs.append(chip_gather(flat_in[i * cut : (i + 1) * cut], length, cores))
    sources = jnp.stack(
        [
            ring_place((spot + offset) % length, length) * cores + (core ^ other)
            for other, offset, _ in acts[0]
        ]
    ).astype(jnp.int32)

    part = tokens // n_sec
    offsets = [offset for other, offset, _ in acts[0] if other == 0]
    mine = lax.dynamic_slice_in_dim(out_grad, col * part, part, 0)
    mine = mine.reshape(part, n_dp, width).transpose(1, 0, 2)
    wanted = jnp.stack(
        [
            ring_place((spot - offset) % length, length) * cores + (core ^ other)
            for other in range(cores)
            for offset in offsets
        ]
    )
    mine = mine[wanted].reshape(cores, length, part, width)
    got = [mine[:, 0]]
    for i, offset in enumerate(offsets[1:]):
        got.append(
            lax.ppermute(mine[:, i + 1], "dp", ring_pairs(length, cores, -offset))
        )
    got = jnp.stack(got, axis=1)
    if cores == 2:
        swap = [(i, i ^ 1) for i in range(n_dp)]
        got = jnp.concatenate([got[0], lax.ppermute(got[1], "dp", swap)], axis=0)
    else:
        got = got[0]
    shares = [got]
    for k in range(1, n_sec):
        shares.append(lax.ppermute(got, "section", [(i, (i + k) % n_sec) for i in range(n_sec)]))
    order = (col - jnp.arange(n_sec)) % n_sec
    grads = jnp.stack(shares)[order]
    grads = grads.transpose(1, 0, 2, 3).reshape(n_dp * tokens, width)
    grad_t = grads.T

    state = [x.T for x in (grad_accum, master_weight, adam_first, adam_second)]
    done = []
    for i in range(pieces):
        done = update_weights(grad_t, [block for _, _, block in acts[i]], state, done, starts[i], tile)
    weight_t, first_t, second_t, rounded_t = done

    places = ((sources // cores - col) % n_sec) * cores + ((sources % cores) ^ core)
    streams = []
    for i in range(chunks):
        dec_parts = [block for _, _, block in decs[i]]
        if length == n_sec:
            partial_out = decode_partial(places, dec_parts, rounded_t, n_sec)
            summed = partial_out[0]
            for k in range(1, n_sec):
                summed = summed + lax.ppermute(
                    partial_out[k], "section", [(s, (s + k) % n_sec) for s in range(n_sec)]
                )
            moved = []
            summed = summed.astype(jnp.bfloat16)
            for j in range(cores):
                pairs = [
                    ((a * cores + b) * n_sec + s, (s * cores + (b ^ j)) * n_sec + a)
                    for a in range(length)
                    for b in range(cores)
                    for s in range(n_sec)
                ]
                moved.append(lax.ppermute(summed[j], ("dp", "section"), pairs))
            if cores == 2:
                flip = core == 1
                moved = [
                    jnp.where(flip, moved[1], moved[0]),
                    jnp.where(flip, moved[0], moved[1]),
                ]
            streams.append(jnp.concatenate(moved, axis=1))
        else:
            partial_out = decode_partial(sources, dec_parts, rounded_t, 1)[0]
            back = lax.all_to_all(partial_out, "dp", 0, 0, tiled=True)
            back = back.transpose(1, 0, 2).reshape(rows, width_all)
            streams.append(lax.psum_scatter(back, "section", scatter_dimension=1, tiled=True))

    resid = lax.dynamic_slice_in_dim(
        residual_in.reshape(rows, width_all), col * share_width, share_width, 1
    ).astype(jnp.float32)
    own_stream = resid + jnp.concatenate(streams, axis=0)
    square_sum = section_sum(jnp.sum(own_stream * own_stream, axis=1, keepdims=True))
    mean_square = square_sum / width_all
    normed = own_stream * lax.rsqrt(mean_square + norm_eps) * norm_gain.astype(jnp.float32)
    decoded = normed.astype(jnp.bfloat16).reshape(steps_count, roll_rows, share_width)
    return (weight_t.T, first_t.T, second_t.T, decoded)


def solution(mesh):
    return jax.shard_map(
        per_device,
        mesh=mesh,
        in_specs=(
            P("dp", "section"),
            P("dp", None),
            P("section", "dp"),
            P("section", "dp"),
            P("section", "dp"),
            P("section", "dp"),
            P(None, "dp", "section"),
            P(None, "dp", None),
            P("section"),
        ),
        out_specs=(
            P("section", "dp"),
            P("section", "dp"),
            P("section", "dp"),
            P(None, "dp", "section"),
        ),
        check_vma=False,
    )
```

```python
import functools
import math

import jax
import jax.numpy as jnp
from jax import lax
from jax.experimental import pallas as pl
from jax.experimental.pallas import tpu as pltpu
from jax.sharding import PartitionSpec as P


beta_first = 0.9
beta_second = 0.95
learn_rate = 0.002
decay_rate = 0.1
adam_eps = 1e-08
norm_eps = 1e-05
bias_first = 1.0 - 0.9**10
bias_second = 1.0 - 0.95**10


def ring_place(index, length):
    return jnp.where(2 * index < length, 2 * index, 2 * (length - index) - 1)


def ring_index(place, length):
    return jnp.where(place % 2 == 0, place // 2, length - (place + 1) // 2)


def ring_order(length):
    return [2 * i if 2 * i < length else 2 * (length - i) - 1 for i in range(length)]


def ring_pairs(length, cores, step):
    order = ring_order(length)
    return [
        (order[i] * cores + c, order[(i + step) % length] * cores + c)
        for i in range(length)
        for c in range(cores)
    ]


def ring_gather(own, length, cores):
    found = [(0, own)]
    up, down = own, own
    for step in range(1, (length - 1) // 2 + 1):
        up = lax.ppermute(up, "dp", ring_pairs(length, cores, 1))
        down = lax.ppermute(down, "dp", ring_pairs(length, cores, -1))
        found += [(-step, up), (step, down)]
    if length % 2 == 0:
        up = lax.ppermute(up, "dp", ring_pairs(length, cores, 1))
        found += [(length // 2, up)]
    return found


def chip_gather(own, length, cores):
    found = [(0, offset, block) for offset, block in ring_gather(own, length, cores)]
    if cores == 2:
        swap = [(i, i ^ 1) for i in range(length * cores)]
        for _, offset, block in list(found):
            found.append((1, offset, lax.ppermute(block, "dp", swap)))
    return found


def pick_tile(size, most):
    fits = [t for t in range(128, most + 1, 128) if size % t == 0]
    return fits[-1] if fits else size


def pick_spans(hidden, split):
    tile = pick_tile(hidden, 512)
    count = hidden // tile
    small = 2 * count // 7
    if not split or small == 0:
        return [hidden]
    return [(count - 2 * small) * tile, small * tile, small * tile]


def update_body(count, grad_ref, *refs):
    acts, (accum, weight, first, second) = refs[:count], refs[count : count + 4]
    w_out, f_out, s_out, r_out = refs[-4:]
    act = jnp.concatenate([ref[...] for ref in acts], axis=0)
    gradient = jnp.dot(grad_ref[...], act, preferred_element_type=jnp.float32) + accum[...]
    first_new = beta_first * first[...] + (1.0 - beta_first) * gradient
    second_new = beta_second * second[...] + (1.0 - beta_second) * gradient * gradient
    scale = jnp.sqrt(second_new * (1.0 / bias_second)) + adam_eps
    update = first_new * (1.0 / bias_first) / scale
    old = weight[...]
    weight_new = old - learn_rate * (update + decay_rate * old)
    w_out[...] = weight_new
    f_out[...] = first_new
    s_out[...] = second_new
    r_out[...] = weight_new.astype(jnp.bfloat16)


def update_weights(grad_t, acts, state, done, start):
    width, hidden = state[0].shape
    span = acts[0].shape[1]
    tile = pick_tile(math.gcd(start, span), 896)
    skip = start // tile
    block = pl.BlockSpec((width, tile), lambda i: (0, i + skip))
    return pl.pallas_call(
        functools.partial(update_body, len(acts)),
        grid=(span // tile,),
        in_specs=[pl.BlockSpec(grad_t.shape, lambda i: (0, 0))]
        + [pl.BlockSpec((act.shape[0], tile), lambda i: (0, i)) for act in acts]
        + [block] * 4
        + [pl.BlockSpec(memory_space=pl.ANY)] * len(done),
        out_specs=[block] * 4,
        out_shape=[jax.ShapeDtypeStruct((width, hidden), jnp.float32)] * 3
        + [jax.ShapeDtypeStruct((width, hidden), jnp.bfloat16)],
        input_output_aliases={5 + len(acts) + i: i for i in range(len(done))},
        cost_estimate=pl.CostEstimate(
            flops=2 * grad_t.shape[1] * width * span,
            bytes_accessed=30 * width * span,
            transcendentals=2 * width * span,
        ),
        name="update_weights",
    )(grad_t, *acts, *state, *done)


def decode_body(count, rows, places, *refs):
    acts, weight, outs = refs[:count], refs[count], refs[count + 1 : -2]
    total, placed = refs[-2:]
    step = pl.program_id(0)
    act = jnp.concatenate([ref[...] for ref in acts], axis=0)
    term = lax.dot_general(
        act, weight[...], (((1,), (1,)), ((), ())), preferred_element_type=jnp.float32
    )

    @pl.when(step == 0)
    def _():
        total[...] = term

    @pl.when(step > 0)
    def _():
        total[...] += term

    @pl.when(step == pl.num_programs(0) - 1)
    def _():
        for block in range(count):
            placed[places[block]] = total[block * rows : (block + 1) * rows, :]
        each = count // len(outs)
        for i, out in enumerate(outs):
            out[...] = placed[i * each : (i + 1) * each]


def decode_partial(places, acts, weight_t, groups):
    width, hidden = weight_t.shape
    tile = pick_tile(hidden, hidden // 2)
    blocks, rows = len(acts), acts[0].shape[0]
    return pl.pallas_call(
        functools.partial(decode_body, blocks, rows),
        grid_spec=pltpu.PrefetchScalarGridSpec(
            num_scalar_prefetch=1,
            grid=(hidden // tile,),
            in_specs=[pl.BlockSpec((act.shape[0], tile), lambda i, p: (0, i)) for act in acts]
            + [pl.BlockSpec((width, tile), lambda i, p: (0, i))],
            out_specs=[pl.BlockSpec((blocks // groups, rows, width), lambda i, p: (0, 0, 0))] * groups,
            scratch_shapes=[
                pltpu.VMEM((blocks * rows, width), jnp.float32),
                pltpu.VMEM((blocks, rows, width), jnp.float32),
            ],
        ),
        out_shape=[jax.ShapeDtypeStruct((blocks // groups, rows, width), jnp.float32)] * groups,
        cost_estimate=pl.CostEstimate(
            flops=2 * blocks * rows * width * hidden,
            bytes_accessed=2 * hidden * (width + blocks * rows),
            transcendentals=0,
        ),
        name="decode_partial",
    )(places, *acts, weight_t)


def section_sum(value):
    count = lax.axis_size("section")
    if count & (count - 1):
        return lax.psum(value, "section")
    step = 1
    while step < count:
        value = value + lax.ppermute(value, "section", [(i, i ^ step) for i in range(count)])
        step *= 2
    return value


def per_device(
    hidden_act,
    out_grad,
    grad_accum,
    master_weight,
    adam_first,
    adam_second,
    decode_in,
    residual_in,
    norm_gain,
):
    n_dp, n_sec = lax.axis_size("dp"), lax.axis_size("section")
    me, col = lax.axis_index("dp"), lax.axis_index("section")
    cores = 2 if n_dp % 2 == 0 else 1
    length = n_dp // cores
    chip, core = me // cores, me % cores
    spot = ring_index(chip, length)
    tokens, width_all = out_grad.shape
    steps_count, roll_rows, hidden_local = decode_in.shape
    rows = steps_count * roll_rows
    width = width_all // n_dp
    share_width = width_all // n_sec

    spans = pick_spans(hidden_local, length == n_sec)
    pieces = len(spans)
    starts = [sum(spans[:i]) for i in range(pieces)]
    chunks = 2 if length == n_sec else 1
    cut = rows // chunks
    acts, decs = [], []
    for i in range(pieces):
        own = hidden_act[:, starts[i] : starts[i] + spans[i]]
        acts.append(chip_gather(own, length, cores))
    flat_in = decode_in.reshape(rows, hidden_local)
    for i in range(chunks):
        decs.append(chip_gather(flat_in[i * cut : (i + 1) * cut], length, cores))
    sources = jnp.stack(
        [
            ring_place((spot + offset) % length, length) * cores + (core ^ other)
            for other, offset, _ in acts[0]
        ]
    ).astype(jnp.int32)

    part = tokens // n_sec
    offsets = [offset for other, offset, _ in acts[0] if other == 0]
    mine = lax.dynamic_slice_in_dim(out_grad, col * part, part, 0)
    mine = mine.reshape(part, n_dp, width).transpose(1, 0, 2)
    wanted = jnp.stack(
        [
            ring_place((spot - offset) % length, length) * cores + (core ^ other)
            for other in range(cores)
            for offset in offsets
        ]
    )
    mine = mine[wanted].reshape(cores, length, part, width)
    got = [mine[:, 0]]
    for i, offset in enumerate(offsets[1:]):
        got.append(
            lax.ppermute(mine[:, i + 1], "dp", ring_pairs(length, cores, -offset))
        )
    got = jnp.stack(got, axis=1)
    if cores == 2:
        swap = [(i, i ^ 1) for i in range(n_dp)]
        got = jnp.concatenate([got[0], lax.ppermute(got[1], "dp", swap)], axis=0)
    else:
        got = got[0]
    shares = [got]
    for k in range(1, n_sec):
        shares.append(lax.ppermute(got, "section", [(i, (i + k) % n_sec) for i in range(n_sec)]))
    order = (col - jnp.arange(n_sec)) % n_sec
    grads = jnp.stack(shares)[order]
    grads = grads.transpose(1, 0, 2, 3).reshape(n_dp * tokens, width)
    grad_t = grads.T

    state = [x.T for x in (grad_accum, master_weight, adam_first, adam_second)]
    done = []
    for i in range(pieces):
        done = update_weights(grad_t, [block for _, _, block in acts[i]], state, done, starts[i])
    weight_t, first_t, second_t, rounded_t = done

    places = ((sources // cores - col) % n_sec) * cores + ((sources % cores) ^ core)
    streams = []
    for i in range(chunks):
        dec_parts = [block for _, _, block in decs[i]]
        if length == n_sec:
            partial_out = decode_partial(places, dec_parts, rounded_t, n_sec)
            summed = partial_out[0]
            for k in range(1, n_sec):
                summed = summed + lax.ppermute(
                    partial_out[k], "section", [(s, (s + k) % n_sec) for s in range(n_sec)]
                )
            moved = []
            summed = summed.astype(jnp.bfloat16)
            for j in range(cores):
                pairs = [
                    ((a * cores + b) * n_sec + s, (s * cores + (b ^ j)) * n_sec + a)
                    for a in range(length)
                    for b in range(cores)
                    for s in range(n_sec)
                ]
                moved.append(lax.ppermute(summed[j], ("dp", "section"), pairs))
            if cores == 2:
                flip = core == 1
                moved = [
                    jnp.where(flip, moved[1], moved[0]),
                    jnp.where(flip, moved[0], moved[1]),
                ]
            streams.append(jnp.concatenate(moved, axis=1))
        else:
            partial_out = decode_partial(sources, dec_parts, rounded_t, 1)[0]
            back = lax.all_to_all(partial_out, "dp", 0, 0, tiled=True)
            back = back.transpose(1, 0, 2).reshape(rows, width_all)
            streams.append(lax.psum_scatter(back, "section", scatter_dimension=1, tiled=True))

    resid = lax.dynamic_slice_in_dim(
        residual_in.reshape(rows, width_all), col * share_width, share_width, 1
    ).astype(jnp.float32)
    own_stream = resid + jnp.concatenate(streams, axis=0)
    square_sum = section_sum(jnp.sum(own_stream * own_stream, axis=1, keepdims=True))
    mean_square = square_sum / width_all
    normed = own_stream * lax.rsqrt(mean_square + norm_eps) * norm_gain.astype(jnp.float32)
    decoded = normed.astype(jnp.bfloat16).reshape(steps_count, roll_rows, share_width)
    return (weight_t.T, first_t.T, second_t.T, decoded)


def solution(mesh):
    return jax.shard_map(
        per_device,
        mesh=mesh,
        in_specs=(
            P("dp", "section"),
            P("dp", None),
            P("section", "dp"),
            P("section", "dp"),
            P("section", "dp"),
            P("section", "dp"),
            P(None, "dp", "section"),
            P(None, "dp", None),
            P("section"),
        ),
        out_specs=(
            P("section", "dp"),
            P("section", "dp"),
            P("section", "dp"),
            P(None, "dp", "section"),
        ),
        check_vma=False,
    )
```
